32 devices in a mesh: expert: 4 (over y, core), shard: 8 (over z, x).
Axes of the slice: x: 2, y: 2, z: 4, core: 2. Of those that a mesh axis runs over, the one named last changes fastest.
Arguments:
- params: float32 [3, 4, 6144, 256], P(None, 'expert', 'shard'), may hold values from -3 to 3
- grads: float32 [3, 4, 6144, 256], P(None, 'expert', 'shard')
- moment: float32 [3, 4, 6144, 256], P(None, 'expert', 'shard'), may hold values from -0.6 to 0.6
- second: float32 [3, 4, 64], P(None, 'expert'), may hold values from 0.002 to 0.2
- step: int32 [1], replicated, may hold values from 1 to 8
- block_map: int32 [256], replicated, may hold values from 0 to 63, never falling along the last dimension, each value on 1 to 8 neighbouring positions
Outputs:
- new_weights: bfloat16 [3, 4, 6144, 256], P(None, 'expert')
- new_moment: float32 [3, 4, 6144, 256], P(None, 'expert', 'shard')
- new_second: float32 [3, 4, 64], P(None, 'expert')
The draws below stay inside these ranges and needn't reach their ends.
Inputs may be any that keep to these rules, and one draw needn't show every extreme that they name: `block_map`: every block holds at least one neuron and at most 8.
All inputs are finite; a program needn't handle non-finite values.
Results may differ from the reference program's by a relative error of at most 0.001.
Values may be sent and summed in bfloat16 or wider, within the bound.
A program may use at most 64 MiB of HBM per device.

```python
import math
import jax
import jax.numpy as jnp
import numpy as np
from jax import lax

D = 6144
NEUR = 256
NBLK = 64
EXPERTS = 4


def draw_grads(key, part):
    keys = jax.random.split(key, 4)
    row_place = jnp.arange(D, dtype=jnp.float32) / D
    expert_place = jnp.arange(EXPERTS, dtype=jnp.float32) / EXPERTS
    noise = jax.random.normal(keys[0], (3, EXPERTS, D, NEUR), jnp.float32)
    row_scale = jnp.power(10.0, 0.5 * row_place + 0.5 * jax.random.uniform(keys[1], (D,), jnp.float32))
    column_scale = jnp.power(10.0, jax.random.uniform(keys[2], (NEUR,), jnp.float32))
    expert_scale = jnp.power(10.0, 0.25 * expert_place + 0.25 * jax.random.uniform(keys[3], (EXPERTS,), jnp.float32))
    return noise * row_scale[None, None, :, None] * column_scale[None, None, None, :] * expert_scale[None, :, None, None]


def block_scale(stream_key, dims, cuts, low, top_value):
    level, own = 1.0, jax.random.fold_in(stream_key, 6)
    for position, blocks in cuts:
        heights = jnp.exp(jax.random.uniform(jax.random.fold_in(own, position), (blocks,), jnp.float32, low / len(cuts), top_value / len(cuts)))
        level = level * jnp.repeat(heights, dims[position] // blocks).reshape([-1 if axis == position else 1 for axis in range(len(dims))])
    return level


def length_profile(count, total, reach, skew):
    loads = [(1 << 20) // math.isqrt(rank ** skew) + 1 for rank in range(2, count + 1)]
    rest, holding = total - reach - (count - 1), [1] * (count - 1)
    while rest > 0:
        candidates = [i for i in range(count - 1) if holding[i] < reach]
        pool, remaining = sum([loads[i] for i in candidates]), rest
        for i in candidates:
            addition = min(reach - holding[i], max(1, remaining * loads[i] // pool), rest)
            holding[i] = holding[i] + addition
            rest = rest - addition
    return np.array([reach] + holding)


def uneven(key, amount, total, reach, skew):
    if amount == 2:
        one = jax.random.randint(key, (), max(1, total - reach), min(reach, total - 1) + 1)
        return jnp.stack([one, total - one])
    sizes = jnp.asarray(length_profile(amount, total, reach, skew), jnp.int32)
    couples = (amount - 1) // 2
    donor, receiver = sizes[1:1 + 2 * couples:2], sizes[2:2 + 2 * couples:2]
    margin = jnp.minimum(donor - 1, reach - receiver)
    moved = jax.random.randint(jax.random.fold_in(key, 1), (couples,), 0, 1 << 20) % (margin + 1)
    sizes = sizes.at[1:1 + 2 * couples:2].set(donor - moved).at[2:2 + 2 * couples:2].set(receiver + moved)
    return sizes[jax.random.permutation(jax.random.fold_in(key, 2), amount)]


def centred(rng, shape, width, reach, pieces=(), kind=jnp.bfloat16):
    level = block_scale(rng, shape, pieces, -0.22, 0.18) if pieces else 1.0
    drawn = jax.random.normal(rng, shape, jnp.float32) * width * level
    return jnp.minimum(jnp.maximum(drawn, -reach), reach).astype(kind)


def setup_inputs(seed: int = 0) -> dict:
    key_list = jax.random.split(jax.random.key(seed), 7)
    return {
        "params": centred(key_list[0], (3, EXPERTS, D, NEUR), 0.5, 3.0, ((1, 4), (2, 8)), jnp.float32),
        "grads": draw_grads(jax.random.fold_in(key_list[6], 71), 0),
        "moment": centred(key_list[2], (3, EXPERTS, D, NEUR), 0.1, 0.6, ((1, 4), (2, 8)), jnp.float32),
        "second": jnp.clip(jnp.exp(math.log(0.2) - 4.6051702 * jax.random.uniform(key_list[3], (3, EXPERTS, NBLK), jnp.float32) ** block_scale(key_list[3], (3, EXPERTS, NBLK), ((1, 4),), -0.2, 0.2)), 0.002, 0.2),
        "step": jax.random.randint(key_list[4], (1,), 1, 9).astype(jnp.int32),
        "block_map": jnp.searchsorted(jnp.cumsum(uneven(key_list[5], NBLK, NEUR, 8, 1)), jnp.arange(NEUR), side="right").astype(jnp.int32),
    }


LEARN_RATE = 0.05
DECAY_WEIGHT = 0.1
BETA_FIRST = 0.9
BETA_SECOND = 0.95
epsilon = 1e-08

def reference(params, grads, moment, second, step, block_map):
    member_table = (block_map[:, None] == jnp.arange(NBLK, dtype=jnp.int32)[None, :]).astype(jnp.float32)
    members = lax.optimization_barrier(jnp.sum(member_table, axis=0))
    squares = lax.optimization_barrier(jnp.sum(grads * grads, axis=2))
    block_sums = jnp.einsum('ken,nb->keb', squares, member_table, precision=lax.Precision.HIGHEST)
    total = jnp.sum(block_sums)
    limit = math.sqrt(3 * EXPERTS * D * NEUR)
    clip = jnp.minimum(1.0, limit / (jnp.sqrt(total) + 1e-06))
    new_second = BETA_SECOND * second + (1.0 - BETA_SECOND) * clip * clip * block_sums / (D * members)
    new_moment = BETA_FIRST * moment + (1.0 - BETA_FIRST) * clip * grads
    step_value = step[0].astype(jnp.float32)
    first_fix = 1.0 - jnp.power(jnp.float32(BETA_FIRST), step_value)
    second_fix = 1.0 - jnp.power(jnp.float32(BETA_SECOND), step_value)
    divisor = jnp.sqrt(new_second / second_fix) + epsilon
    by_neuron = jnp.einsum('keb,nb->ken', divisor, member_table, precision=lax.Precision.HIGHEST)
    updated = params * (1.0 - LEARN_RATE * DECAY_WEIGHT) - LEARN_RATE * (new_moment / first_fix) / by_neuron[:, :, None, :]
    return (updated.astype(jnp.bfloat16), new_moment, new_second)
```

```python
import functools
import itertools
import math

import jax
import jax.numpy as jnp
from jax import lax
from jax.experimental import pallas as pl
from jax.experimental.pallas import tpu as pltpu
from jax.sharding import PartitionSpec as P

LEARN_RATE = 0.05
DECAY_WEIGHT = 0.1
BETA_FIRST = 0.9
BETA_SECOND = 0.95
epsilon = 1e-08
MESH = pl.DeviceIdType.MESH
LANES = 128
STRIP = 64
CUTS = 1


def ring_position(shard, n):
    if n % 2:
        return shard
    row, side = shard // 2, shard % 2
    return jnp.where(side == 0, row, n - 1 - row)


def ring_shard(position, n):
    position = lax.rem(position + 2 * n, n)
    if n % 2:
        return position
    return jnp.where(position < n // 2, 2 * position, 2 * (n - 1 - position) + 1)


def split3(x):
    high = x.astype(jnp.bfloat16)
    rest = x - high.astype(jnp.float32)
    middle = rest.astype(jnp.bfloat16)
    low = (rest - middle.astype(jnp.float32)).astype(jnp.bfloat16)
    return jnp.concatenate([high, middle, low], axis=0)


def gather_columns(x, onehot, dims):
    n = x.shape[0]
    out = lax.dot_general(split3(x), onehot, (dims, ((), ())), preferred_element_type=jnp.float32)
    return out[:n] + out[n : 2 * n] + out[2 * n :]


def kernel(
    experts,
    shards,
    limit,
    params,
    grads,
    moment,
    second,
    step,
    block_map,
    weights,
    new_moment,
    new_second,
    g_buf,
    pm_buf,
    s_buf,
    map_buf,
    tile,
    total_row,
    tiles,
    totals,
    load_sem,
    small_sem,
    tile_sem,
    total_sem,
    ring_send,
    ring_recv,
):
    e = lax.axis_index("expert")
    s = lax.axis_index("shard")
    devices = experts * shards
    me = e * shards + s
    mats, rows, neurons = g_buf.shape
    width = rows * shards
    folds = neurons // LANES
    backward = s < shards // 2

    def far_first(t, own, count):
        t = jnp.where(backward, count - 2 - t, t)
        return t + (t >= own).astype(jnp.int32)

    barrier = pltpu.get_barrier_semaphore()

    def greet(t, carry):
        other = far_first(t, me, devices)
        pl.semaphore_signal(
            barrier,
            inc=1,
            device_id=(lax.div(other, shards), lax.rem(other, shards)),
            device_id_type=MESH,
        )
        return carry

    lax.fori_loop(0, devices - 1, greet, 0)

    map_load = pltpu.make_async_copy(block_map, map_buf, small_sem.at[0])
    second_load = pltpu.make_async_copy(second, s_buf, small_sem.at[1])
    for k in range(mats):
        pltpu.make_async_copy(grads.at[k], g_buf.at[k], load_sem.at[k]).start()
    map_load.start()
    second_load.start()

    blocks = second.shape[2]
    map_load.wait()
    own_blocks = map_buf[...]
    table = (
        lax.broadcasted_iota(jnp.int32, (blocks, neurons), 0) == own_blocks
    ).astype(jnp.bfloat16)
    same = lax.dot_general(
        table, table, (((0,), (0,)), ((), ())), preferred_element_type=jnp.float32
    ).astype(jnp.bfloat16)
    members = lax.dot_general(
        jnp.ones((8, neurons), jnp.bfloat16),
        table,
        (((1,), (1,)), ((), ())),
        preferred_element_type=jnp.float32,
    )[:mats]
    members_here = lax.dot_general(
        jnp.ones((8, neurons), jnp.bfloat16),
        same,
        (((1,), (0,)), ((), ())),
        preferred_element_type=jnp.float32,
    )[:mats]
    second_load.wait()
    second_here = gather_columns(s_buf[:, 0, :], table, ((1,), (0,)))
    step_value = jnp.full((1, LANES), step[0].astype(jnp.float32))
    first_fix = 1.0 - jnp.power(jnp.full((1, LANES), BETA_FIRST, jnp.float32), step_value)
    second_fix = 1.0 - jnp.power(jnp.full((1, LANES), BETA_SECOND, jnp.float32), step_value)
    first_fix = first_fix[:, :1]
    second_fix = second_fix[:, :1]

    squares = []
    for k in range(mats):
        pltpu.make_async_copy(grads.at[k], g_buf.at[k], load_sem.at[k]).wait()
        if k == mats - 1:
            for i in range(mats):
                pltpu.make_async_copy(params.at[i], pm_buf.at[0, i], load_sem.at[mats + i]).start()
                pltpu.make_async_copy(moment.at[i], pm_buf.at[1, i], load_sem.at[mats + i]).start()

        def add_squares(i, acc, k=k):
            g = g_buf[k, pl.ds(pl.multiple_of(i * STRIP, STRIP), STRIP), :]
            return acc + jnp.sum((g * g).reshape(STRIP // 8, 8, neurons), axis=0)

        acc = lax.fori_loop(0, rows // STRIP, add_squares, jnp.zeros((8, neurons), jnp.float32), unroll=2)
        squares.append(jnp.sum(acc, axis=0, keepdims=True))
    parts = [sq[:, f * LANES : (f + 1) * LANES] for f in range(folds) for sq in squares]
    own_total = functools.reduce(lambda a, b: a + b, parts)
    pad = tile.shape[0] - len(parts)
    if pad:
        parts.append(jnp.zeros((pad, LANES), jnp.float32))
    own_tile = jnp.concatenate(parts, axis=0)
    tile[...] = own_tile
    total_row[...] = own_total
    tiles[s] = own_tile

    def blank(i, carry):
        totals[e * shards + i] = jnp.zeros((1, LANES), jnp.float32)
        return carry

    lax.fori_loop(0, shards, blank, 0)

    pl.semaphore_wait(barrier, devices - 1)

    def start_total(t, carry):
        other_s = jnp.where(backward, shards - 1 - t, t)
        for d in range(1, experts):
            pltpu.make_async_remote_copy(
                src_ref=total_row,
                dst_ref=totals.at[me],
                send_sem=total_sem.at[0],
                recv_sem=total_sem.at[1],
                device_id=(lax.rem(e + d, experts), other_s),
                device_id_type=MESH,
            ).start()
        return carry

    def start_tile(t, carry):
        pltpu.make_async_remote_copy(
            src_ref=tile,
            dst_ref=tiles.at[s],
            send_sem=tile_sem.at[0],
            recv_sem=tile_sem.at[1],
            device_id=(e, far_first(t, s, shards)),
            device_id_type=MESH,
        ).start()
        return carry

    def wait_bytes(ref, sem):
        pltpu.make_async_copy(ref, ref, sem).wait()

    lax.fori_loop(0, shards, start_total, 0)
    lax.fori_loop(0, shards - 1, start_tile, 0)
    other_tiles = tiles.at[pl.ds(0, shards - 1)]
    other_totals = totals.at[pl.ds(0, devices - shards)]
    wait_bytes(other_tiles, tile_sem.at[1])
    wait_bytes(other_totals, total_sem.at[1])

    all_tile = jnp.sum(tiles[...], axis=0)
    total = jnp.sum(totals[...], axis=0) + jnp.sum(all_tile, axis=0, keepdims=True)
    total = jnp.sum(total, axis=1, keepdims=True)
    square = jnp.concatenate(
        [all_tile[f * mats : (f + 1) * mats] for f in range(folds)], axis=1
    )
    sums_here = gather_columns(square, same, ((1,), (0,)))
    clip = jnp.minimum(1.0, limit / (jnp.sqrt(total) + 1e-06))
    updated_here = BETA_SECOND * second_here + (1.0 - BETA_SECOND) * clip * clip * sums_here / (
        width * members_here
    )
    by_neuron = jnp.sqrt(updated_here / second_fix) + epsilon
    rate = LEARN_RATE / (first_fix * by_neuron)
    grad_scale = (1.0 - BETA_FIRST) * clip

    place = ring_position(s, shards)
    half = rows // 2
    right = ring_shard(place + 1, shards)
    left = ring_shard(place - 1, shards)
    far, near = shards // 2, (shards - 1) // 2
    hops = ((far, near), (near, far))

    piece = half // CUTS

    def ring_copy(way, hop, part, k, q, arriving):
        back = hop + (1 if arriving else 0)
        origin = ring_shard(place - back if way == 0 else place + back, shards)
        first = pl.multiple_of(origin * rows + part * half + q * piece, piece)
        block = weights.at[k, pl.ds(first, piece), :]
        index = ((2 * hop + part) * mats + k) * CUTS + q
        return pltpu.make_async_remote_copy(
            src_ref=block,
            dst_ref=block,
            send_sem=ring_send,
            recv_sem=ring_recv.at[way, index],
            device_id=(e, right if way == 0 else left),
            device_id_type=MESH,
        )

    for k in range(mats):
        wait_bytes(pm_buf.at[:, k], load_sem.at[mats + k])
        rate_k = rate[k : k + 1]
        for part in range(2):
            for q in range(CUTS):

                def update(i, carry, k=k, part=part, q=q, rate_k=rate_k):
                    at = pl.multiple_of(part * half + q * piece + i * STRIP, STRIP)
                    strip = pl.ds(at, STRIP)
                    value = BETA_FIRST * pm_buf[1, k, strip, :] + grad_scale * g_buf[k, strip, :]
                    new_moment[k, strip, :] = value
                    out = pm_buf[0, k, strip, :] * (1.0 - LEARN_RATE * DECAY_WEIGHT) - rate_k * value
                    weights[k, pl.ds(pl.multiple_of(s * rows + at, STRIP), STRIP), :] = out.astype(
                        jnp.bfloat16
                    )
                    return carry

                lax.fori_loop(0, piece // STRIP, update, 0, unroll=2)
                for way in range(2):
                    if hops[way][part] > 0:
                        ring_copy(way, 0, part, k, q, False).start()

    block_sums = gather_columns(square, table, ((1,), (1,)))
    updated = BETA_SECOND * s_buf[:, 0, :] + (1.0 - BETA_SECOND) * clip * clip * block_sums / (
        width * members
    )
    for k in range(mats):
        new_second[k] = updated[k : k + 1]

    for hop in range(far):
        for k, part, q in itertools.product(range(mats), range(2), range(CUTS)):
            for way in range(2):
                if hop < hops[way][part]:
                    ring_copy(way, hop, part, k, q, True).wait_recv()
                    if hop + 1 < hops[way][part]:
                        ring_copy(way, hop + 1, part, k, q, False).start()
    wait_bytes(weights.at[:, pl.ds(0, width - rows), :], ring_send)
    wait_bytes(other_tiles, tile_sem.at[0])
    wait_bytes(other_totals, total_sem.at[0])


def store_kernel(weights, moment, second, weights_out, moment_out, second_out, sem):
    mats = weights.shape[0]
    for k in range(mats):
        pltpu.make_async_copy(weights.at[k], weights_out.at[k], sem.at[0]).start()
    for k in range(mats):
        pltpu.make_async_copy(moment.at[k], moment_out.at[k], sem.at[1]).start()
    second_copy = pltpu.make_async_copy(second, second_out, sem.at[2])
    second_copy.start()
    pltpu.make_async_copy(weights, weights_out, sem.at[0]).wait()
    pltpu.make_async_copy(moment, moment_out, sem.at[1]).wait()
    second_copy.wait()


def body(params, grads, moment, second, step, block_map):
    experts, shards = lax.axis_size("expert"), lax.axis_size("shard")
    mats, own, rows, neurons = params.shape
    blocks = second.shape[2]
    width = rows * shards
    devices = experts * shards
    limit = math.sqrt(mats * experts * own * width * neurons)
    flat = (mats, own * rows, neurons)
    far = max(shards // 2, 1)
    tile_rows = -(-mats * (neurons // LANES) // 8) * 8
    hbm = pl.BlockSpec(memory_space=pltpu.HBM)
    vmem = pl.BlockSpec(memory_space=pltpu.VMEM)
    smem = pl.BlockSpec(memory_space=pltpu.SMEM)
    dma = pltpu.SemaphoreType.DMA
    shapes = (
        jax.ShapeDtypeStruct((mats, width, neurons), jnp.bfloat16),
        jax.ShapeDtypeStruct(flat, jnp.float32),
        jax.ShapeDtypeStruct((mats, own, blocks), jnp.float32),
    )
    results = pl.pallas_call(
        functools.partial(kernel, experts, shards, limit),
        out_shape=tuple(pltpu.VMEM(shape.shape, shape.dtype) for shape in shapes),
        in_specs=[hbm, hbm, hbm, hbm, smem, hbm],
        out_specs=(vmem, vmem, vmem),
        scratch_shapes=[
            pltpu.VMEM(flat, jnp.float32),
            pltpu.VMEM((2, *flat), jnp.float32),
            pltpu.VMEM((mats, own, blocks), jnp.float32),
            pltpu.VMEM((1, neurons), jnp.int32),
            pltpu.VMEM((tile_rows, LANES), jnp.float32),
            pltpu.VMEM((1, LANES), jnp.float32),
            pltpu.VMEM((shards, tile_rows, LANES), jnp.float32),
            pltpu.VMEM((devices, 1, LANES), jnp.float32),
            dma((2 * mats,)),
            dma((2,)),
            dma((2,)),
            dma((2,)),
            dma(()),
            dma((2, 2 * far * mats * CUTS)),
        ],
        compiler_params=pltpu.CompilerParams(
            collective_id=0, has_side_effects=True, vmem_limit_bytes=46 * 1024 * 1024
        ),
    )(
        params.reshape(flat),
        grads.reshape(flat),
        moment.reshape(flat),
        second,
        step,
        block_map.reshape(1, neurons),
    )
    weights, new_moment, new_second = pl.pallas_call(
        store_kernel,
        out_shape=shapes,
        in_specs=[vmem, vmem, vmem],
        out_specs=(hbm, hbm, hbm),
        scratch_shapes=[dma((3,))],
        compiler_params=pltpu.CompilerParams(vmem_limit_bytes=8 * 1024 * 1024),
    )(*results)
    return (
        weights.reshape(mats, own, width, neurons),
        new_moment.reshape(mats, own, rows, neurons),
        new_second,
    )


def solution(mesh):
    placed = (
        P(None, "expert", "shard", None),
        P(None, "expert", "shard", None),
        P(None, "expert", "shard", None),
        P(None, "expert", None),
        P(),
        P(),
    )
    return jax.shard_map(
        body,
        mesh=mesh,
        in_specs=placed,
        out_specs=(
            P(None, "expert", None, None),
            P(None, "expert", "shard", None),
            P(None, "expert", None),
        ),
        check_vma=False,
    )
```

```python
import functools
import itertools
import math

import jax
import jax.numpy as jnp
from jax import lax
from jax.experimental import pallas as pl
from jax.experimental.pallas import tpu as pltpu
from jax.sharding import PartitionSpec as P

LEARN_RATE = 0.05
DECAY_WEIGHT = 0.1
BETA_FIRST = 0.9
BETA_SECOND = 0.95
epsilon = 1e-08
MESH = pl.DeviceIdType.MESH
LANES = 128
STRIP = 64


def ring_position(shard, n):
    if n % 2:
        return shard
    row, side = shard // 2, shard % 2
    return jnp.where(side == 0, row, n - 1 - row)


def ring_order(n):
    if n % 2:
        return list(range(n))
    return list(range(0, n, 2)) + list(range(n - 1, 0, -2))


def ring_shard(position, n):
    position = lax.rem(position + 2 * n, n)
    if n % 2:
        return position
    return jnp.where(position < n // 2, 2 * position, 2 * (n - 1 - position) + 1)


def split3(x):
    high = x.astype(jnp.bfloat16)
    rest = x - high.astype(jnp.float32)
    middle = rest.astype(jnp.bfloat16)
    low = (rest - middle.astype(jnp.float32)).astype(jnp.bfloat16)
    return jnp.concatenate([high, middle, low], axis=0)


def gather_columns(x, onehot, dims):
    n = x.shape[0]
    out = lax.dot_general(split3(x), onehot, (dims, ((), ())), preferred_element_type=jnp.float32)
    return out[:n] + out[n : 2 * n] + out[2 * n :]


def kernel(
    experts,
    shards,
    limit,
    params,
    grads,
    moment,
    second,
    step,
    block_map,
    weights0,
    weights1,
    new_moment,
    new_second,
    g_buf,
    pm_buf,
    s_buf,
    map_buf,
    tile,
    total_row,
    tiles,
    totals,
    load_sem,
    small_sem,
    tile_sem,
    total_sem,
):
    e = lax.axis_index("expert")
    s = lax.axis_index("shard")
    devices = experts * shards
    me = e * shards + s
    mats, rows, neurons = g_buf.shape
    width = rows * shards
    folds = neurons // LANES
    half = rows // 2
    strip = math.gcd(STRIP, half)
    backward = s < shards // 2

    def far_first(t, own, count):
        t = jnp.where(backward, count - 2 - t, t)
        return t + (t >= own).astype(jnp.int32)

    for k in range(mats):
        pltpu.make_async_copy(grads.at[k], g_buf.at[k], load_sem.at[k]).start()

    barrier = pltpu.get_barrier_semaphore()

    def greet(t, carry):
        other = far_first(t, me, devices)
        pl.semaphore_signal(
            barrier,
            inc=1,
            device_id=(lax.div(other, shards), lax.rem(other, shards)),
            device_id_type=MESH,
        )
        return carry

    lax.fori_loop(0, devices - 1, greet, 0)

    map_load = pltpu.make_async_copy(block_map, map_buf, small_sem.at[0])
    second_load = pltpu.make_async_copy(second, s_buf, small_sem.at[1])
    map_load.start()
    second_load.start()

    blocks = second.shape[2]
    map_load.wait()
    own_blocks = map_buf[...]
    table = (
        lax.broadcasted_iota(jnp.int32, (blocks, neurons), 0) == own_blocks
    ).astype(jnp.bfloat16)
    same = lax.dot_general(
        table, table, (((0,), (0,)), ((), ())), preferred_element_type=jnp.float32
    ).astype(jnp.bfloat16)
    members = lax.dot_general(
        jnp.ones((8, neurons), jnp.bfloat16),
        table,
        (((1,), (1,)), ((), ())),
        preferred_element_type=jnp.float32,
    )[:mats]
    members_here = lax.dot_general(
        jnp.ones((8, neurons), jnp.bfloat16),
        same,
        (((1,), (0,)), ((), ())),
        preferred_element_type=jnp.float32,
    )[:mats]
    second_load.wait()
    second_here = gather_columns(s_buf[:, 0, :], table, ((1,), (0,)))
    step_value = jnp.full((1, LANES), step[0].astype(jnp.float32))
    first_fix = 1.0 - jnp.power(jnp.full((1, LANES), BETA_FIRST, jnp.float32), step_value)
    second_fix = 1.0 - jnp.power(jnp.full((1, LANES), BETA_SECOND, jnp.float32), step_value)
    first_fix = first_fix[:, :1]
    second_fix = second_fix[:, :1]

    squares = []
    for k in range(mats):
        pltpu.make_async_copy(grads.at[k], g_buf.at[k], load_sem.at[k]).wait()
        if k == mats - 1:
            for i in range(mats):
                pltpu.make_async_copy(params.at[i], pm_buf.at[0, i], load_sem.at[mats + i]).start()
                pltpu.make_async_copy(moment.at[i], pm_buf.at[1, i], load_sem.at[mats + i]).start()

        def add_squares(i, acc, k=k):
            g = g_buf[k, pl.ds(pl.multiple_of(i * strip, strip), strip), :]
            return acc + jnp.sum((g * g).reshape(strip // 8, 8, neurons), axis=0)

        acc = lax.fori_loop(0, rows // strip, add_squares, jnp.zeros((8, neurons), jnp.float32), unroll=2)
        squares.append(jnp.sum(acc, axis=0, keepdims=True))
    parts = [sq[:, f * LANES : (f + 1) * LANES] for f in range(folds) for sq in squares]
    own_total = functools.reduce(lambda a, b: a + b, parts)
    pad = tile.shape[0] - len(parts)
    if pad:
        parts.append(jnp.zeros((pad, LANES), jnp.float32))
    own_tile = jnp.concatenate(parts, axis=0)
    tile[...] = own_tile
    total_row[...] = own_total
    tiles[s] = own_tile

    def blank(i, carry):
        totals[e * shards + i] = jnp.zeros((1, LANES), jnp.float32)
        return carry

    lax.fori_loop(0, shards, blank, 0)

    pl.semaphore_wait(barrier, devices - 1)

    def start_total(t, carry):
        other_s = jnp.where(backward, shards - 1 - t, t)
        for d in range(1, experts):
            pltpu.make_async_remote_copy(
                src_ref=total_row,
                dst_ref=totals.at[me],
                send_sem=total_sem.at[0],
                recv_sem=total_sem.at[1],
                device_id=(lax.rem(e + d, experts), other_s),
                device_id_type=MESH,
            ).start()
        return carry

    def start_tile(t, carry):
        pltpu.make_async_remote_copy(
            src_ref=tile,
            dst_ref=tiles.at[s],
            send_sem=tile_sem.at[0],
            recv_sem=tile_sem.at[1],
            device_id=(e, far_first(t, s, shards)),
            device_id_type=MESH,
        ).start()
        return carry

    def wait_bytes(ref, sem):
        pltpu.make_async_copy(ref, ref, sem).wait()

    lax.fori_loop(0, shards, start_total, 0)
    lax.fori_loop(0, shards - 1, start_tile, 0)
    other_tiles = tiles.at[pl.ds(0, shards - 1)]
    other_totals = totals.at[pl.ds(0, devices - shards)]
    wait_bytes(other_tiles, tile_sem.at[1])
    wait_bytes(other_totals, total_sem.at[1])

    all_tile = jnp.sum(tiles[...], axis=0)
    total = jnp.sum(totals[...], axis=0) + jnp.sum(all_tile, axis=0, keepdims=True)
    total = jnp.sum(total, axis=1, keepdims=True)
    square = jnp.concatenate(
        [all_tile[f * mats : (f + 1) * mats] for f in range(folds)], axis=1
    )
    sums_here = gather_columns(square, same, ((1,), (0,)))
    clip = jnp.minimum(1.0, limit / (jnp.sqrt(total) + 1e-06))
    updated_here = BETA_SECOND * second_here + (1.0 - BETA_SECOND) * clip * clip * sums_here / (
        width * members_here
    )
    by_neuron = jnp.sqrt(updated_here / second_fix) + epsilon
    rate = LEARN_RATE / (first_fix * by_neuron)
    grad_scale = (1.0 - BETA_FIRST) * clip

    def fresh(p, g, m, rate_k):
        value = BETA_FIRST * m + grad_scale * g
        out = p * (1.0 - LEARN_RATE * DECAY_WEIGHT) - rate_k * value
        return value, out.astype(jnp.bfloat16)

    for k in range(mats):
        wait_bytes(pm_buf.at[:, k], load_sem.at[mats + k])
        for part in range(2):

            def update(i, carry, k=k, part=part):
                at = pl.multiple_of(part * half + i * strip, strip)
                here = pl.ds(at, strip)
                value, out = fresh(
                    pm_buf[0, k, here, :], g_buf[k, here, :], pm_buf[1, k, here, :], rate[k : k + 1]
                )
                new_moment[k, here, :] = value
                (weights0, weights1)[part][k, pl.ds(pl.multiple_of(i * strip, strip), strip), :] = out
                return carry

            lax.fori_loop(0, half // strip, update, 0, unroll=2 if half // strip % 2 == 0 else 1)

    block_sums = gather_columns(square, table, ((1,), (1,)))
    updated = BETA_SECOND * s_buf[:, 0, :] + (1.0 - BETA_SECOND) * clip * clip * block_sums / (
        width * members
    )
    for k in range(mats):
        new_second[k] = updated[k : k + 1]

    wait_bytes(other_tiles, tile_sem.at[0])
    wait_bytes(other_totals, total_sem.at[0])


def moved(n):
    return pl.CostEstimate(flops=0, bytes_accessed=n, transcendentals=0)


def own_store(shards, w0, w1, moment, second, out, moment_out, second_out, sem):
    s = lax.axis_index("shard")
    half = w0.shape[1]
    copies = []
    for p, w in enumerate((w0, w1)):
        at = pl.multiple_of(s * 2 * half + p * half, half)
        copies.append(pltpu.make_async_copy(w, out.at[:, pl.ds(at, half)], sem.at[p]))
    copies.append(pltpu.make_async_copy(moment, moment_out, sem.at[2]))
    copies.append(pltpu.make_async_copy(second, second_out, sem.at[3]))
    for c in copies:
        c.start()
    for c in copies:
        c.wait()


def hop_store(shards, hop, which, *refs):
    n = len(which)
    pieces, out, sem = refs[:n], refs[n + 1], refs[n + 2]
    half = pieces[0].shape[1]
    place = ring_position(lax.axis_index("shard"), shards)
    copies = []
    for i, (way, part) in enumerate(which):
        origin = ring_shard(place - hop if way == 0 else place + hop, shards)
        at = pl.multiple_of(origin * 2 * half + part * half, half)
        copies.append(pltpu.make_async_copy(pieces[i], out.at[:, pl.ds(at, half)], sem.at[i]))
    for c in copies:
        c.start()
    for c in copies:
        c.wait()


def body(params, grads, moment, second, step, block_map):
    experts, shards = lax.axis_size("expert"), lax.axis_size("shard")
    mats, own, rows, neurons = params.shape
    blocks = second.shape[2]
    width = rows * shards
    devices = experts * shards
    limit = math.sqrt(mats * experts * own * width * neurons)
    flat = (mats, own * rows, neurons)
    tile_rows = -(-mats * (neurons // LANES) // 8) * 8
    hbm = pl.BlockSpec(memory_space=pltpu.HBM)
    vmem = pl.BlockSpec(memory_space=pltpu.VMEM)
    smem = pl.BlockSpec(memory_space=pltpu.SMEM)
    dma = pltpu.SemaphoreType.DMA
    shapes = (
        jax.ShapeDtypeStruct((mats, rows // 2, neurons), jnp.bfloat16),
        jax.ShapeDtypeStruct((mats, rows // 2, neurons), jnp.bfloat16),
        jax.ShapeDtypeStruct(flat, jnp.float32),
        jax.ShapeDtypeStruct((mats, own, blocks), jnp.float32),
    )
    results = pl.pallas_call(
        functools.partial(kernel, experts, shards, limit),
        out_shape=tuple(pltpu.VMEM(shape.shape, shape.dtype) for shape in shapes),
        in_specs=[hbm, hbm, hbm, hbm, smem, hbm],
        out_specs=(vmem, vmem, vmem, vmem),
        scratch_shapes=[
            pltpu.VMEM(flat, jnp.float32),
            pltpu.VMEM((2, *flat), jnp.float32),
            pltpu.VMEM((mats, own, blocks), jnp.float32),
            pltpu.VMEM((1, neurons), jnp.int32),
            pltpu.VMEM((tile_rows, LANES), jnp.float32),
            pltpu.VMEM((1, LANES), jnp.float32),
            pltpu.VMEM((shards, tile_rows, LANES), jnp.float32),
            pltpu.VMEM((devices, 1, LANES), jnp.float32),
            dma((2 * mats,)),
            dma((2,)),
            dma((2,)),
            dma((2,)),
        ],
        compiler_params=pltpu.CompilerParams(
            collective_id=0, has_side_effects=True, vmem_limit_bytes=56 * 1024 * 1024
        ),
    )(
        params.reshape(flat),
        grads.reshape(flat),
        moment.reshape(flat),
        second,
        step,
        block_map.reshape(1, neurons),
    )
    w0, w1, m_new, s_new = results
    full = jax.ShapeDtypeStruct((mats, width, neurons), jnp.bfloat16)
    ring = ring_order(shards)
    ways = tuple(
        [(ring[p], ring[(p + step) % shards]) for p in range(shards)] for step in (1, -1)
    )
    far, near = shards // 2, (shards - 1) // 2
    hops = ((far, near), (near, far))
    row_bytes = mats * neurons * 2
    weights, new_moment, new_second = pl.pallas_call(
        functools.partial(own_store, shards),
        out_shape=(full, shapes[2], shapes[3]),
        in_specs=[vmem] * 4,
        out_specs=(hbm, hbm, hbm),
        scratch_shapes=[dma((4,))],
        cost_estimate=moved(6 * rows * row_bytes // 2),
        compiler_params=pltpu.CompilerParams(vmem_limit_bytes=4 * 1024 * 1024),
    )(w0, w1, m_new, s_new)
    now = {(way, part): (w0, w1)[part] for way in range(2) for part in range(2)}
    for hop in range(far):
        now = {
            (way, part): lax.ppermute(now[way, part], "shard", ways[way])
            for part in range(2)
            for way in range(2)
            if hop < hops[way][part]
        }
        which = tuple(now)
        weights = pl.pallas_call(
            functools.partial(hop_store, shards, hop + 1, which),
            out_shape=full,
            in_specs=[vmem] * len(which) + [hbm],
            out_specs=hbm,
            scratch_shapes=[dma((len(which),))],
            input_output_aliases={len(which): 0},
            cost_estimate=moved(2 * len(which) * (rows // 2) * row_bytes),
            compiler_params=pltpu.CompilerParams(vmem_limit_bytes=4 * 1024 * 1024),
        )(*now.values(), weights)
    return (
        weights.reshape(mats, own, width, neurons),
        new_moment.reshape(mats, own, rows, neurons),
        new_second,
    )


def solution(mesh):
    placed = (
        P(None, "expert", "shard", None),
        P(None, "expert", "shard", None),
        P(None, "expert", "shard", None),
        P(None, "expert", None),
        P(),
        P(),
    )
    return jax.shard_map(
        body,
        mesh=mesh,
        in_specs=placed,
        out_specs=(
            P(None, "expert", None, None),
            P(None, "expert", "shard", None),
            P(None, "expert", None),
        ),
        check_vma=False,
    )
```

```python
import functools
import math

import jax
import jax.numpy as jnp
from jax import lax
from jax.experimental import pallas as pl
from jax.experimental.pallas import tpu as pltpu
from jax.sharding import PartitionSpec as P


LEARN_RATE = 0.05
DECAY_WEIGHT = 0.1
BETA_FIRST = 0.9
BETA_SECOND = 0.95
epsilon = 1e-08
MESH = pl.DeviceIdType.MESH
LANES = 128
STRIP = 64
PIECES = 4


def ring_position(shard, n):
    if n % 2:
        return shard
    row, side = shard // 2, shard % 2
    return jnp.where(side == 0, row, n - 1 - row)


def ring_order(n):
    if n % 2:
        return list(range(n))
    return list(range(0, n, 2)) + list(range(n - 1, 0, -2))


def ring_shard(position, n):
    position = lax.rem(position + 2 * n, n)
    if n % 2:
        return position
    return jnp.where(position < n // 2, 2 * position, 2 * (n - 1 - position) + 1)


def split3(x):
    high = x.astype(jnp.bfloat16)
    rest = x - high.astype(jnp.float32)
    middle = rest.astype(jnp.bfloat16)
    low = (rest - middle.astype(jnp.float32)).astype(jnp.bfloat16)
    return jnp.concatenate([high, middle, low], axis=0)


def gather_columns(x, onehot, dims):
    n = x.shape[0]
    out = lax.dot_general(split3(x), onehot, (dims, ((), ())), preferred_element_type=jnp.float32)
    return out[:n] + out[n : 2 * n] + out[2 * n :]


def kernel(
    experts,
    shards,
    limit,
    params,
    grads,
    moment,
    second,
    step,
    block_map,
    *refs,
):
    pieces = refs[:PIECES]
    (
        new_moment,
        new_second,
        g_buf,
        pm_buf,
        s_buf,
        map_buf,
        tile,
        total_row,
        tiles,
        totals,
        load_sem,
        small_sem,
        tile_sem,
        total_sem,
    ) = refs[PIECES:]
    e = lax.axis_index("expert")
    s = lax.axis_index("shard")
    devices = experts * shards
    me = e * shards + s
    mats, rows, neurons = g_buf.shape
    width = rows * shards
    folds = neurons // LANES
    length = rows // PIECES
    strip = math.gcd(STRIP, length)
    backward = s < shards // 2

    def far_first(t, own, count):
        t = jnp.where(backward, count - 2 - t, t)
        return t + (t >= own).astype(jnp.int32)

    for k in range(mats):
        pltpu.make_async_copy(grads.at[k], g_buf.at[k], load_sem.at[k]).start()

    barrier = pltpu.get_barrier_semaphore()

    def greet(t, carry):
        other = far_first(t, me, devices)
        pl.semaphore_signal(
            barrier,
            inc=1,
            device_id=(lax.div(other, shards), lax.rem(other, shards)),
            device_id_type=MESH,
        )
        return carry

    lax.fori_loop(0, devices - 1, greet, 0)

    map_load = pltpu.make_async_copy(block_map, map_buf, small_sem.at[0])
    second_load = pltpu.make_async_copy(second, s_buf, small_sem.at[1])
    map_load.start()
    second_load.start()

    blocks = second.shape[2]
    map_load.wait()
    own_blocks = map_buf[...]
    table = (
        lax.broadcasted_iota(jnp.int32, (blocks, neurons), 0) == own_blocks
    ).astype(jnp.bfloat16)
    same = lax.dot_general(
        table, table, (((0,), (0,)), ((), ())), preferred_element_type=jnp.float32
    ).astype(jnp.bfloat16)
    members = lax.dot_general(
        jnp.ones((8, neurons), jnp.bfloat16),
        table,
        (((1,), (1,)), ((), ())),
        preferred_element_type=jnp.float32,
    )[:mats]
    members_here = lax.dot_general(
        jnp.ones((8, neurons), jnp.bfloat16),
        same,
        (((1,), (0,)), ((), ())),
        preferred_element_type=jnp.float32,
    )[:mats]
    second_load.wait()
    second_here = gather_columns(s_buf[:, 0, :], table, ((1,), (0,)))
    step_value = jnp.full((1, LANES), step[0].astype(jnp.float32))
    first_fix = 1.0 - jnp.power(jnp.full((1, LANES), BETA_FIRST, jnp.float32), step_value)
    second_fix = 1.0 - jnp.power(jnp.full((1, LANES), BETA_SECOND, jnp.float32), step_value)
    first_fix = first_fix[:, :1]
    second_fix = second_fix[:, :1]

    squares = []
    for k in range(mats):
        pltpu.make_async_copy(grads.at[k], g_buf.at[k], load_sem.at[k]).wait()
        if k == mats - 1:
            for i in range(mats):
                pltpu.make_async_copy(params.at[i], pm_buf.at[0, i], load_sem.at[mats + i]).start()
                pltpu.make_async_copy(moment.at[i], pm_buf.at[1, i], load_sem.at[mats + i]).start()

        def add_squares(i, acc, k=k):
            g = g_buf[k, pl.ds(pl.multiple_of(i * strip, strip), strip), :]
            return acc + jnp.sum((g * g).reshape(strip // 8, 8, neurons), axis=0)

        acc = lax.fori_loop(0, rows // strip, add_squares, jnp.zeros((8, neurons), jnp.float32), unroll=2)
        squares.append(jnp.sum(acc, axis=0, keepdims=True))
    parts = [sq[:, f * LANES : (f + 1) * LANES] for f in range(folds) for sq in squares]
    own_total = functools.reduce(lambda a, b: a + b, parts)
    pad = tile.shape[0] - len(parts)
    if pad:
        parts.append(jnp.zeros((pad, LANES), jnp.float32))
    own_tile = jnp.concatenate(parts, axis=0)
    tile[...] = own_tile
    total_row[...] = own_total
    tiles[s] = own_tile

    def blank(i, carry):
        totals[e * shards + i] = jnp.zeros((1, LANES), jnp.float32)
        return carry

    lax.fori_loop(0, shards, blank, 0)

    pl.semaphore_wait(barrier, devices - 1)

    def start_total(t, carry):
        other_s = jnp.where(backward, shards - 1 - t, t)
        for d in range(1, experts):
            pltpu.make_async_remote_copy(
                src_ref=total_row,
                dst_ref=totals.at[me],
                send_sem=total_sem.at[0],
                recv_sem=total_sem.at[1],
                device_id=(lax.rem(e + d, experts), other_s),
                device_id_type=MESH,
            ).start()
        return carry

    def start_tile(t, carry):
        pltpu.make_async_remote_copy(
            src_ref=tile,
            dst_ref=tiles.at[s],
            send_sem=tile_sem.at[0],
            recv_sem=tile_sem.at[1],
            device_id=(e, far_first(t, s, shards)),
            device_id_type=MESH,
        ).start()
        return carry

    def wait_bytes(ref, sem):
        pltpu.make_async_copy(ref, ref, sem).wait()

    lax.fori_loop(0, shards, start_total, 0)
    lax.fori_loop(0, shards - 1, start_tile, 0)
    other_tiles = tiles.at[pl.ds(0, shards - 1)]
    other_totals = totals.at[pl.ds(0, devices - shards)]
    wait_bytes(other_tiles, tile_sem.at[1])
    wait_bytes(other_totals, total_sem.at[1])

    all_tile = jnp.sum(tiles[...], axis=0)
    total = jnp.sum(totals[...], axis=0) + jnp.sum(all_tile, axis=0, keepdims=True)
    total = jnp.sum(total, axis=1, keepdims=True)
    square = jnp.concatenate(
        [all_tile[f * mats : (f + 1) * mats] for f in range(folds)], axis=1
    )
    sums_here = gather_columns(square, same, ((1,), (0,)))
    clip = jnp.minimum(1.0, limit / (jnp.sqrt(total) + 1e-06))
    updated_here = BETA_SECOND * second_here + (1.0 - BETA_SECOND) * clip * clip * sums_here / (
        width * members_here
    )
    by_neuron = jnp.sqrt(updated_here / second_fix) + epsilon
    rate = LEARN_RATE / (first_fix * by_neuron)
    grad_scale = (1.0 - BETA_FIRST) * clip

    def fresh(p, g, m, rate_k):
        value = BETA_FIRST * m + grad_scale * g
        out = p * (1.0 - LEARN_RATE * DECAY_WEIGHT) - rate_k * value
        return value, out.astype(jnp.bfloat16)

    for k in range(mats):
        wait_bytes(pm_buf.at[:, k], load_sem.at[mats + k])
        for q in range(PIECES):

            def update(i, carry, k=k, q=q):
                at = pl.multiple_of(i * strip, strip)
                here = pl.ds(pl.multiple_of(q * length + at, strip), strip)
                value, out = fresh(
                    pm_buf[0, k, here, :], g_buf[k, here, :], pm_buf[1, k, here, :], rate[k : k + 1]
                )
                new_moment[k, here, :] = value
                pieces[q][k, pl.ds(at, strip), :] = out
                return carry

            lax.fori_loop(0, length // strip, update, 0, unroll=True)

    block_sums = gather_columns(square, table, ((1,), (1,)))
    updated = BETA_SECOND * s_buf[:, 0, :] + (1.0 - BETA_SECOND) * clip * clip * block_sums / (
        width * members
    )
    for k in range(mats):
        new_second[k] = updated[k : k + 1]

    wait_bytes(other_tiles, tile_sem.at[0])
    wait_bytes(other_totals, total_sem.at[0])


def moved(n):
    return pl.CostEstimate(flops=0, bytes_accessed=n, transcendentals=0)


def own_store(*refs):
    pieces = refs[:PIECES]
    moment, second, out, moment_out, second_out, sem = refs[PIECES:]
    s = lax.axis_index("shard")
    length = pieces[0].shape[1]
    copies = []
    for q, piece in enumerate(pieces):
        at = pl.multiple_of((s * PIECES + q) * length, length)
        copies.append(pltpu.make_async_copy(piece, out.at[:, pl.ds(at, length)], sem.at[q]))
    copies.append(pltpu.make_async_copy(moment, moment_out, sem.at[PIECES]))
    copies.append(pltpu.make_async_copy(second, second_out, sem.at[PIECES + 1]))
    for c in copies:
        c.start()
    for c in copies:
        c.wait()


def hop_store(shards, hop, which, *refs):
    n = len(which)
    pieces, out, sem = refs[:n], refs[n + 1], refs[n + 2]
    length = pieces[0].shape[1]
    place = ring_position(lax.axis_index("shard"), shards)
    copies = []
    for i, (way, q) in enumerate(which):
        origin = ring_shard(place - hop if way == 0 else place + hop, shards)
        at = pl.multiple_of((origin * PIECES + q) * length, length)
        copies.append(pltpu.make_async_copy(pieces[i], out.at[:, pl.ds(at, length)], sem.at[i]))
    for c in copies:
        c.start()
    for c in copies:
        c.wait()


def moved(n):
    return pl.CostEstimate(flops=0, bytes_accessed=n, transcendentals=0)


def ring_starts(n):
    far, near = n // 2, (n - 1) // 2
    return [
        (hop, way, (j + way * PIECES // 2) % PIECES)
        for hop in range(far)
        for j in range(PIECES)
        for way in range(2)
        if hop < (far if j < PIECES // 2 else near)
    ]


def step_body(params, grads, moment, second, step, block_map):
    experts, shards = lax.axis_size("expert"), lax.axis_size("shard")
    mats, own, rows, neurons = params.shape
    blocks = second.shape[2]
    width = rows * shards
    devices = experts * shards
    limit = math.sqrt(mats * experts * own * width * neurons)
    flat = (mats, own * rows, neurons)
    tile_rows = -(-mats * (neurons // LANES) // 8) * 8
    hbm = pl.BlockSpec(memory_space=pltpu.HBM)
    vmem = pl.BlockSpec(memory_space=pltpu.VMEM)
    smem = pl.BlockSpec(memory_space=pltpu.SMEM)
    dma = pltpu.SemaphoreType.DMA
    piece = jax.ShapeDtypeStruct((mats, own * rows // PIECES, neurons), jnp.bfloat16)
    shapes = (piece,) * PIECES + (
        jax.ShapeDtypeStruct(flat, jnp.float32),
        jax.ShapeDtypeStruct((mats, own, blocks), jnp.float32),
    )
    results = pl.pallas_call(
        functools.partial(kernel, experts, shards, limit),
        out_shape=tuple(pltpu.VMEM(shape.shape, shape.dtype) for shape in shapes),
        in_specs=[hbm, hbm, hbm, hbm, smem, hbm],
        out_specs=(vmem,) * len(shapes),
        scratch_shapes=[
            pltpu.VMEM(flat, jnp.float32),
            pltpu.VMEM((2, *flat), jnp.float32),
            pltpu.VMEM((mats, own, blocks), jnp.float32),
            pltpu.VMEM((1, neurons), jnp.int32),
            pltpu.VMEM((tile_rows, LANES), jnp.float32),
            pltpu.VMEM((1, LANES), jnp.float32),
            pltpu.VMEM((shards, tile_rows, LANES), jnp.float32),
            pltpu.VMEM((devices, 1, LANES), jnp.float32),
            dma((2 * mats,)),
            dma((2,)),
            dma((2,)),
            dma((2,)),
        ],
        compiler_params=pltpu.CompilerParams(
            collective_id=0, has_side_effects=True, vmem_limit_bytes=56 * 1024 * 1024
        ),
    )(
        params.reshape(flat),
        grads.reshape(flat),
        moment.reshape(flat),
        second,
        step,
        block_map.reshape(1, neurons),
    )
    full = jax.ShapeDtypeStruct((mats, width, neurons), jnp.bfloat16)
    ring = ring_order(shards)
    ways = tuple(
        [(ring[p], ring[(p + step) % shards]) for p in range(shards)] for step in (1, -1)
    )
    row_bytes = mats * neurons * 2
    weights, new_moment, new_second = pl.pallas_call(
        own_store,
        out_shape=(full, *shapes[PIECES:]),
        in_specs=[vmem] * len(shapes),
        out_specs=(hbm, hbm, hbm),
        scratch_shapes=[dma((PIECES + 2,))],
        cost_estimate=moved(6 * rows * row_bytes // 2),
        compiler_params=pltpu.CompilerParams(vmem_limit_bytes=4 * 1024 * 1024),
    )(*results)
    now = {(way, q): results[q] for way in range(2) for q in range(PIECES)}
    starts = ring_starts(shards)
    far = starts[-1][0] + 1
    arrived = []
    for n, (hop, way, q) in enumerate(starts):
        now[way, q] = lax.ppermute(now[way, q], "shard", ways[way])
        arrived.append((way, q))
        last = starts[n + 1 : n + 2]
        if not last or last[0][0] > hop or (hop == far - 1 and len(arrived) == 2):
            which = tuple(arrived)
            weights = pl.pallas_call(
                functools.partial(hop_store, shards, hop + 1, which),
                out_shape=full,
                in_specs=[vmem] * len(which) + [hbm],
                out_specs=hbm,
                scratch_shapes=[dma((len(which),))],
                input_output_aliases={len(which): 0},
                cost_estimate=moved(2 * len(which) * (rows // PIECES) * row_bytes),
                compiler_params=pltpu.CompilerParams(vmem_limit_bytes=4 * 1024 * 1024),
            )(*[now[w] for w in which], weights)
            arrived = []
    return (
        weights.reshape(mats, own, width, neurons),
        new_moment.reshape(mats, own, rows, neurons),
        new_second,
    )


def solution(mesh):
    placed = (
        P(None, "expert", "shard", None),
        P(None, "expert", "shard", None),
        P(None, "expert", "shard", None),
        P(None, "expert", None),
        P(),
        P(),
    )
    return jax.shard_map(
        step_body,
        mesh=mesh,
        in_specs=placed,
        out_specs=(
            P(None, "expert", None, None),
            P(None, "expert", "shard", None),
            P(None, "expert", None),
        ),
        check_vma=False,
    )
```

```python
import functools
import math

import jax
import jax.numpy as jnp
from jax import lax
from jax.experimental import pallas as pl
from jax.experimental.pallas import tpu as pltpu
from jax.sharding import PartitionSpec as P


LEARN_RATE = 0.05
DECAY_WEIGHT = 0.1
BETA_FIRST = 0.9
BETA_SECOND = 0.95
epsilon = 1e-08
MESH = pl.DeviceIdType.MESH
LANES = 128
STRIP = 64
PIECES = 6


def ring_position(shard, n):
    if n % 2:
        return shard
    row, side = shard // 2, shard % 2
    return jnp.where(side == 0, row, n - 1 - row)


def ring_order(n):
    if n % 2:
        return list(range(n))
    return list(range(0, n, 2)) + list(range(n - 1, 0, -2))


def ring_shard(position, n):
    position = lax.rem(position + 2 * n, n)
    if n % 2:
        return position
    return jnp.where(position < n // 2, 2 * position, 2 * (n - 1 - position) + 1)


def split3(x):
    high = x.astype(jnp.bfloat16)
    rest = x - high.astype(jnp.float32)
    middle = rest.astype(jnp.bfloat16)
    low = (rest - middle.astype(jnp.float32)).astype(jnp.bfloat16)
    return jnp.concatenate([high, middle, low], axis=0)


def gather_columns(x, onehot, dims):
    n = x.shape[0]
    out = lax.dot_general(split3(x), onehot, (dims, ((), ())), preferred_element_type=jnp.float32)
    return out[:n] + out[n : 2 * n] + out[2 * n :]


def kernel(
    experts,
    shards,
    limit,
    params,
    grads,
    moment,
    second,
    step,
    block_map,
    *refs,
):
    pieces = refs[:PIECES]
    (
        square_out,
        clip_out,
        g_buf,
        pm_buf,
        s_buf,
        map_buf,
        tile,
        total_row,
        tiles,
        totals,
        load_sem,
        small_sem,
        tile_sem,
        total_sem,
    ) = refs[PIECES:]
    e = lax.axis_index("expert")
    s = lax.axis_index("shard")
    devices = experts * shards
    me = e * shards + s
    mats, rows, neurons = g_buf.shape
    width = rows * shards
    folds = neurons // LANES
    length = rows // PIECES
    strip = math.gcd(STRIP, length)
    backward = s < shards // 2

    def far_first(t, own, count):
        t = jnp.where(backward, count - 2 - t, t)
        return t + (t >= own).astype(jnp.int32)

    for k in range(mats):
        pltpu.make_async_copy(grads.at[k], g_buf.at[k], load_sem.at[k]).start()

    barrier = pltpu.get_barrier_semaphore()

    def greet(t, carry):
        other = far_first(t, me, devices)
        pl.semaphore_signal(
            barrier,
            inc=1,
            device_id=(lax.div(other, shards), lax.rem(other, shards)),
            device_id_type=MESH,
        )
        return carry

    lax.fori_loop(0, devices - 1, greet, 0)

    map_load = pltpu.make_async_copy(block_map, map_buf, small_sem.at[0])
    second_load = pltpu.make_async_copy(second, s_buf, small_sem.at[1])
    map_load.start()
    second_load.start()

    blocks = second.shape[2]
    map_load.wait()
    own_blocks = map_buf[...]
    table = (
        lax.broadcasted_iota(jnp.int32, (blocks, neurons), 0) == own_blocks
    ).astype(jnp.bfloat16)
    same = lax.dot_general(
        table, table, (((0,), (0,)), ((), ())), preferred_element_type=jnp.float32
    ).astype(jnp.bfloat16)
    members_here = lax.dot_general(
        jnp.ones((8, neurons), jnp.bfloat16),
        same,
        (((1,), (0,)), ((), ())),
        preferred_element_type=jnp.float32,
    )[:mats]
    second_load.wait()
    second_here = gather_columns(s_buf[:, 0, :], table, ((1,), (0,)))
    step_value = jnp.full((1, LANES), step[0].astype(jnp.float32))
    first_fix = 1.0 - jnp.power(jnp.full((1, LANES), BETA_FIRST, jnp.float32), step_value)
    second_fix = 1.0 - jnp.power(jnp.full((1, LANES), BETA_SECOND, jnp.float32), step_value)
    first_fix = first_fix[:, :1]
    second_fix = second_fix[:, :1]

    def blank(i, carry):
        totals[e * shards + i] = jnp.zeros((1, LANES), jnp.float32)
        return carry

    lax.fori_loop(0, shards, blank, 0)

    squares = []
    for k in range(mats):
        pltpu.make_async_copy(grads.at[k], g_buf.at[k], load_sem.at[k]).wait()
        if k == mats - 1:
            for i in range(mats):
                pltpu.make_async_copy(params.at[i], pm_buf.at[0, i], load_sem.at[mats + i]).start()
                pltpu.make_async_copy(moment.at[i], pm_buf.at[1, i], load_sem.at[mats + i]).start()

        def add_squares(i, acc, k=k):
            g = g_buf[k, pl.ds(pl.multiple_of(i * strip, strip), strip), :]
            return acc + jnp.sum((g * g).reshape(strip // 8, 8, neurons), axis=0)

        acc = lax.fori_loop(0, rows // strip, add_squares, jnp.zeros((8, neurons), jnp.float32), unroll=2)
        squares.append(jnp.sum(acc, axis=0, keepdims=True))
    parts = [sq[:, f * LANES : (f + 1) * LANES] for f in range(folds) for sq in squares]
    own_total = functools.reduce(lambda a, b: a + b, parts)
    total_row[...] = own_total

    pl.semaphore_wait(barrier, devices - 1)

    def start_total(t, carry):
        other_s = jnp.where(backward, shards - 1 - t, t)
        for d in range(1, experts):
            pltpu.make_async_remote_copy(
                src_ref=total_row,
                dst_ref=totals.at[me],
                send_sem=total_sem.at[0],
                recv_sem=total_sem.at[1],
                device_id=(lax.rem(e + d, experts), other_s),
                device_id_type=MESH,
            ).start()
        return carry

    def start_tile(t, carry):
        pltpu.make_async_remote_copy(
            src_ref=tile,
            dst_ref=tiles.at[s],
            send_sem=tile_sem.at[0],
            recv_sem=tile_sem.at[1],
            device_id=(e, far_first(t, s, shards)),
            device_id_type=MESH,
        ).start()
        return carry

    def wait_bytes(ref, sem):
        pltpu.make_async_copy(ref, ref, sem).wait()

    lax.fori_loop(0, shards, start_total, 0)
    pad = tile.shape[0] - len(parts)
    if pad:
        parts.append(jnp.zeros((pad, LANES), jnp.float32))
    own_tile = jnp.concatenate(parts, axis=0)
    tile[...] = own_tile
    tiles[s] = own_tile
    lax.fori_loop(0, shards - 1, start_tile, 0)
    other_tiles = tiles.at[pl.ds(0, shards - 1)]
    other_totals = totals.at[pl.ds(0, devices - shards)]
    wait_bytes(other_tiles, tile_sem.at[1])
    wait_bytes(other_totals, total_sem.at[1])

    all_tile = jnp.sum(tiles[...], axis=0)
    total = jnp.sum(totals[...], axis=0) + jnp.sum(all_tile, axis=0, keepdims=True)
    total = jnp.sum(total, axis=1, keepdims=True)
    square = jnp.concatenate(
        [all_tile[f * mats : (f + 1) * mats] for f in range(folds)], axis=1
    )
    sums_here = gather_columns(square, same, ((1,), (0,)))
    clip = jnp.minimum(1.0, limit / (jnp.sqrt(total) + 1e-06))
    updated_here = BETA_SECOND * second_here + (1.0 - BETA_SECOND) * clip * clip * sums_here / (
        width * members_here
    )
    by_neuron = jnp.sqrt(updated_here / second_fix) + epsilon
    rate = LEARN_RATE / (first_fix * by_neuron)
    grad_scale = (1.0 - BETA_FIRST) * clip

    def fresh(p, g, m, rate_k):
        value = BETA_FIRST * m + grad_scale * g
        out = p * (1.0 - LEARN_RATE * DECAY_WEIGHT) - rate_k * value
        return out.astype(jnp.bfloat16)

    for k in range(mats):
        wait_bytes(pm_buf.at[:, k], load_sem.at[mats + k])
        for q in range(PIECES):

            def update(i, carry, k=k, q=q):
                at = pl.multiple_of(i * strip, strip)
                here = pl.ds(pl.multiple_of(q * length + at, strip), strip)
                pieces[q][k, pl.ds(at, strip), :] = fresh(
                    pm_buf[0, k, here, :], g_buf[k, here, :], pm_buf[1, k, here, :], rate[k : k + 1]
                )
                return carry

            lax.fori_loop(0, length // strip, update, 0, unroll=True)

    square_out[...] = square
    clip_out[...] = jnp.broadcast_to(clip, (1, LANES))

    wait_bytes(other_tiles, tile_sem.at[0])
    wait_bytes(other_totals, total_sem.at[0])


def moved(n):
    return pl.CostEstimate(flops=0, bytes_accessed=n, transcendentals=0)


def own_store(shards, *refs):
    pieces = refs[:PIECES]
    (
        square,
        clip_row,
        grads,
        moment,
        second,
        block_map,
        out,
        moment_out,
        second_out,
        gm_buf,
        value_buf,
        second_buf,
        load_sem,
        store_sem,
    ) = refs[PIECES:]
    s = lax.axis_index("shard")
    mats, rows, neurons = value_buf.shape
    length = pieces[0].shape[1]
    strip = math.gcd(STRIP, rows)
    copies = []
    for q, piece in enumerate(pieces):
        at = pl.multiple_of((s * PIECES + q) * length, length)
        copies.append(pltpu.make_async_copy(piece, out.at[:, pl.ds(at, length)], store_sem.at[q]))
    for c in copies:
        c.start()
    for k in range(mats):
        pltpu.make_async_copy(grads.at[k], gm_buf.at[0, k], load_sem.at[k]).start()
        pltpu.make_async_copy(moment.at[k], gm_buf.at[1, k], load_sem.at[k]).start()

    def wait_bytes(ref, sem):
        pltpu.make_async_copy(ref, ref, sem).wait()

    clip = clip_row[:, :1]
    table = (
        lax.broadcasted_iota(jnp.int32, (second.shape[2], neurons), 0) == block_map[...]
    ).astype(jnp.bfloat16)
    members = lax.dot_general(
        jnp.ones((8, neurons), jnp.bfloat16),
        table,
        (((1,), (1,)), ((), ())),
        preferred_element_type=jnp.float32,
    )[:mats]
    block_sums = gather_columns(square[...], table, ((1,), (1,)))
    updated = BETA_SECOND * second[:, 0, :] + (1.0 - BETA_SECOND) * clip * clip * block_sums / (
        rows * shards * members
    )
    for k in range(mats):
        second_buf[k] = updated[k : k + 1]
    copies.append(pltpu.make_async_copy(second_buf, second_out, store_sem.at[PIECES]))
    copies[-1].start()
    grad_scale = (1.0 - BETA_FIRST) * clip
    for k in range(mats):
        wait_bytes(gm_buf.at[:, k], load_sem.at[k])

        def update(i, carry, k=k):
            here = pl.ds(pl.multiple_of(i * strip, strip), strip)
            value_buf[k, here, :] = BETA_FIRST * gm_buf[1, k, here, :] + grad_scale * gm_buf[0, k, here, :]
            return carry

        lax.fori_loop(0, rows // strip, update, 0)
        pltpu.make_async_copy(value_buf.at[k], moment_out.at[k], store_sem.at[PIECES + 1]).start()
    wait_bytes(value_buf, store_sem.at[PIECES + 1])
    for c in copies:
        c.wait()


def hop_store(shards, hop, which, *refs):
    n = len(which)
    pieces, out, sem = refs[:n], refs[n + 1], refs[n + 2]
    length = pieces[0].shape[1]
    place = ring_position(lax.axis_index("shard"), shards)
    copies = []
    for i, (way, q) in enumerate(which):
        origin = ring_shard(place - hop if way == 0 else place + hop, shards)
        at = pl.multiple_of((origin * PIECES + q) * length, length)
        copies.append(pltpu.make_async_copy(pieces[i], out.at[:, pl.ds(at, length)], sem.at[i]))
    for c in copies:
        c.start()
    for c in copies:
        c.wait()


def moved(n):
    return pl.CostEstimate(flops=0, bytes_accessed=n, transcendentals=0)


def ring_starts(n):
    far, near = n // 2, (n - 1) // 2
    return [
        (hop, way, (j + way * PIECES // 2) % PIECES)
        for hop in range(far)
        for j in range(PIECES)
        for way in range(2)
        if hop < (far if j < PIECES // 2 else near)
    ]


def step_body(params, grads, moment, second, step, block_map):
    experts, shards = lax.axis_size("expert"), lax.axis_size("shard")
    mats, own, rows, neurons = params.shape
    blocks = second.shape[2]
    width = rows * shards
    devices = experts * shards
    limit = math.sqrt(mats * experts * own * width * neurons)
    flat = (mats, own * rows, neurons)
    tile_rows = -(-mats * (neurons // LANES) // 8) * 8
    hbm = pl.BlockSpec(memory_space=pltpu.HBM)
    vmem = pl.BlockSpec(memory_space=pltpu.VMEM)
    smem = pl.BlockSpec(memory_space=pltpu.SMEM)
    dma = pltpu.SemaphoreType.DMA
    piece = jax.ShapeDtypeStruct((mats, own * rows // PIECES, neurons), jnp.bfloat16)
    small = (
        jax.ShapeDtypeStruct((mats, neurons), jnp.float32),
        jax.ShapeDtypeStruct((1, LANES), jnp.float32),
    )
    shapes = (piece,) * PIECES + small
    arrays = (params.reshape(flat), grads.reshape(flat), moment.reshape(flat))
    blocks_row = block_map.reshape(1, neurons)
    results = pl.pallas_call(
        functools.partial(kernel, experts, shards, limit),
        out_shape=tuple(pltpu.VMEM(shape.shape, shape.dtype) for shape in shapes),
        in_specs=[hbm, hbm, hbm, hbm, smem, hbm],
        out_specs=(vmem,) * len(shapes),
        scratch_shapes=[
            pltpu.VMEM(flat, jnp.float32),
            pltpu.VMEM((2, *flat), jnp.float32),
            pltpu.VMEM((mats, own, blocks), jnp.float32),
            pltpu.VMEM((1, neurons), jnp.int32),
            pltpu.VMEM((tile_rows, LANES), jnp.float32),
            pltpu.VMEM((1, LANES), jnp.float32),
            pltpu.VMEM((shards, tile_rows, LANES), jnp.float32),
            pltpu.VMEM((devices, 1, LANES), jnp.float32),
            dma((2 * mats,)),
            dma((2,)),
            dma((2,)),
            dma((2,)),
        ],
        compiler_params=pltpu.CompilerParams(
            collective_id=0, has_side_effects=True, vmem_limit_bytes=56 * 1024 * 1024
        ),
    )(
        *arrays,
        second,
        step,
        blocks_row,
    )
    full = jax.ShapeDtypeStruct((mats, width, neurons), jnp.bfloat16)
    ring = ring_order(shards)
    ways = tuple(
        [(ring[p], ring[(p + step) % shards]) for p in range(shards)] for step in (1, -1)
    )
    row_bytes = mats * neurons * 2
    weights, new_moment, new_second = pl.pallas_call(
        functools.partial(own_store, shards),
        out_shape=(
            full,
            jax.ShapeDtypeStruct(flat, jnp.float32),
            jax.ShapeDtypeStruct(second.shape, jnp.float32),
        ),
        in_specs=[vmem] * len(shapes) + [hbm, hbm, vmem, vmem],
        out_specs=(hbm, hbm, hbm),
        scratch_shapes=[
            pltpu.VMEM((2, *flat), jnp.float32),
            pltpu.VMEM(flat, jnp.float32),
            pltpu.VMEM(second.shape, jnp.float32),
            dma((mats,)),
            dma((PIECES + 2,)),
        ],
        cost_estimate=moved(7 * rows * row_bytes),
        compiler_params=pltpu.CompilerParams(vmem_limit_bytes=12 * 1024 * 1024),
    )(*results, *arrays[1:], second, blocks_row)
    now = {(way, q): results[q] for way in range(2) for q in range(PIECES)}
    starts = ring_starts(shards)
    far = starts[-1][0] + 1
    arrived = []
    for n, (hop, way, q) in enumerate(starts):
        now[way, q] = lax.ppermute(now[way, q], "shard", ways[way])
        arrived.append((way, q))
        last = starts[n + 1 : n + 2]
        if not last or last[0][0] > hop or (hop == far - 1 and len(arrived) == 2):
            which = tuple(arrived)
            weights = pl.pallas_call(
                functools.partial(hop_store, shards, hop + 1, which),
                out_shape=full,
                in_specs=[vmem] * len(which) + [hbm],
                out_specs=hbm,
                scratch_shapes=[dma((len(which),))],
                input_output_aliases={len(which): 0},
                cost_estimate=moved(2 * len(which) * (rows // PIECES) * row_bytes),
                compiler_params=pltpu.CompilerParams(vmem_limit_bytes=4 * 1024 * 1024),
            )(*[now[w] for w in which], weights)
            arrived = []
    return (
        weights.reshape(mats, own, width, neurons),
        new_moment.reshape(mats, own, rows, neurons),
        new_second,
    )


def solution(mesh):
    placed = (
        P(None, "expert", "shard", None),
        P(None, "expert", "shard", None),
        P(None, "expert", "shard", None),
        P(None, "expert", None),
        P(),
        P(),
    )
    return jax.shard_map(
        step_body,
        mesh=mesh,
        in_specs=placed,
        out_specs=(
            P(None, "expert", None, None),
            P(None, "expert", "shard", None),
            P(None, "expert", None),
        ),
        check_vma=False,
    )
```
